32 devices in a mesh: team: 4 (over x, core), row: 2 (over y), col: 4 (over z).
Axes of the slice: x: 2, y: 2, z: 4, core: 2. Of those that a mesh axis runs over, the one named last changes fastest.
Arguments:
- old_tiles: bfloat16 [4, 192, 256, 256], P('team', ('row', 'col')), may hold values from -4 to 4
- remap: int32 [4, 192], P('team', ('row', 'col')), may hold values from 0 to 255, as said below
- pivot_cols: bfloat16 [4, 5120, 1024], P('team', ('row', 'col')), may hold values from -6 to 6
- pivot_order: int32 [4, 2, 512], P('team'), may hold values from 0 to 511, each once within a row
- pivot_pattern: int32 [4, 2, 256], P('team'), may hold values 0 or 1
- block_inverses: float32 [4, 2, 3, 256], P('team'), may hold values from -0.05 to 0.05
- delays: int32 [4, 2], P('team'), may hold values from 0 to 128
Outputs:
- parent: float32 [2, 2048, 4096], P('row', 'team', 'col')
- second_panel: float32 [4, 5120, 512], P('team', ('row', 'col'))
The draws below stay inside these ranges and needn't reach their ends.
Inputs may be any that keep to these rules, and one draw needn't show every extreme that they name: `remap`: tiles that one device holds go to at most 8 distinct owners, the owner of tile (i, j) being the device at row i // 8, column j // 4; at most 3 of one device's tiles go to one owner, and in every front some owner receives exactly 3 tiles from every device.
All inputs are finite; a program needn't handle non-finite values. No bound on the sum of `pivot_pattern` on one device may be relied on, other than what follows from the above.
Results may differ from the reference program's by a relative error of at most 0.0003.
Values may be sent and summed in bfloat16 or wider, within the bound.
No kernel may reach another device: no remote copies, remote signals or barrier semaphores. Data moves between devices by JAX's collectives and lax.ppermute only.
A program may use at most 128 MiB of HBM per device.

```python
import jax
import jax.numpy as jnp
from jax import lax

TILE = 256
PANEL = 512
NF = 5120
OLD_DEV = 24
NC = 4096
NCT = 16
TEAMS = 4
OLD_TILES = 192
HOLD = 8
TRD = 8
TCD = 4
N_ROW = 2
N_COL = 4


def draw_remap(key, part):
    peers = N_ROW * N_COL

    def one_team(team_key):
        key_busy, key_perm, key_slot = jax.random.split(team_key, 3)
        busiest = jax.random.randint(key_busy, (), 0, peers)

        def sender_order(sender_key):
            rest = jax.random.permutation(sender_key, peers - 1) + 1
            return jnp.concatenate([jnp.zeros((1,), jnp.int32), rest.astype(jnp.int32)])
        offsets = jax.vmap(sender_order)(jax.random.split(key_perm, peers))
        chosen = offsets[:, jnp.arange(OLD_DEV, dtype=jnp.int32) % HOLD]
        owners = (busiest + chosen) % peers
        slots = jax.random.randint(key_slot, (peers, OLD_DEV), 0, TRD * TCD)
        owner_row = owners // N_COL
        owner_col = owners % N_COL
        tile_row = owner_row * TRD + slots // TCD
        tile_col = owner_col * TCD + slots % TCD
        return (tile_row * NCT + tile_col).reshape(peers * OLD_DEV).astype(jnp.int32)
    return jax.vmap(one_team)(jax.random.split(jax.random.fold_in(key, 7), TEAMS))


def touch_ends(values, stream_key, least, largest):
    longest = values.shape.index(max(values.shape))
    spots = []
    for shift in (0, 1):
        where = [jax.random.randint(jax.random.fold_in(stream_key, axis), (), 0, length) for axis, length in enumerate(values.shape)]
        where[longest] = (where[longest] + shift) % values.shape[longest]
        spots.append(tuple(where))
    return values.at[spots[0]].set(least).at[spots[1]].set(largest)


def block_levels(rng, shape, cuts, low, top_value):
    factor_of = 1.0
    for dim, shards_of in cuts:
        draws = jax.random.uniform(jax.random.fold_in(jax.random.fold_in(rng, 6), dim), (shards_of,), jnp.float32, low / len(cuts), top_value / len(cuts))
        factor_of = factor_of * jnp.repeat(jnp.exp(draws), shape[dim] // shards_of).reshape((-1,) + (1,) * (len(shape) - 1 - dim))
    return factor_of


def gaussian(key, dims, width, limit, cuts=(), kind=jnp.bfloat16):
    loudness = block_levels(key, dims, cuts, -0.22, 0.18) if cuts else 1.0
    entries = jax.random.normal(key, dims, jnp.float32) * width * loudness
    return jnp.minimum(jnp.maximum(entries, -limit), limit).astype(kind)


def setup_inputs(seed: int = 0) -> dict:
    keys = jax.random.split(jax.random.key(seed), 8)
    return {
        "old_tiles": gaussian(keys[0], (TEAMS, OLD_TILES, TILE, TILE), 0.6, 4.0, ((0, 4), (1, 8))),
        "remap": draw_remap(jax.random.fold_in(keys[7], 71), 0),
        "pivot_cols": gaussian(keys[2], (TEAMS, NF, 2 * PANEL), 1.0, 6.0, ((0, 4), (1, 8))),
        "pivot_order": jax.vmap(lambda own: jax.random.permutation(own, PANEL))(jax.random.split(keys[3], TEAMS * 2)).reshape((TEAMS, 2, PANEL)).astype(jnp.int32),
        "pivot_pattern": touch_ends((jax.random.randint(keys[4], (TEAMS, 2, PANEL // 2), 0, 2) < 1).astype(jnp.int32), jax.random.fold_in(keys[4], 1), 0, 1),
        "block_inverses": gaussian(keys[5], (TEAMS, 2, 3, PANEL // 2), 0.02, 0.05, ((0, 4),), jnp.float32),
        "delays": touch_ends(jax.random.randint(keys[6], (TEAMS, 2), 0, PANEL // 4 + 1), jax.random.fold_in(keys[6], 1), 0, (PANEL // 4 + 1) - 1).astype(jnp.int32),
    }


def make_coeffs(inverses, pattern, delay):
    half_panel = PANEL // 2
    positions = jnp.arange(PANEL, dtype=jnp.int32)
    active = (positions < PANEL - delay).astype(jnp.float32)
    active_lo = active[:half_panel]
    active_hi = active[half_panel:]
    diag_one = inverses[0] * active_lo
    off_diag = inverses[1] * pattern.astype(jnp.float32) * active_lo * active_hi
    diag_two = inverses[2] * active_hi
    return diag_one, off_diag, diag_two


def scale_pivots(columns, coeffs):
    diag_one, off_diag, diag_two = coeffs
    half_panel = PANEL // 2
    left_half = columns[:, :half_panel]
    right_half = columns[:, half_panel:]
    return jnp.concatenate([left_half * diag_one + right_half * off_diag, left_half * off_diag + right_half * diag_two], axis=1)


def one_front(old_tiles, remap, pivot_cols, pivot_order, pivot_pattern, block_inverses, delays):
    old_flat = old_tiles.astype(jnp.float32).reshape(OLD_TILES, TILE * TILE)
    summed = jax.ops.segment_sum(old_flat, remap, num_segments=NCT * NCT)
    front_c = summed.reshape(NCT, NCT, TILE, TILE).transpose(0, 2, 1, 3).reshape(NC, NC)
    widened = pivot_cols.astype(jnp.float32)
    first = jnp.take(widened[:, :PANEL], pivot_order[0], axis=1)
    scaled_one = scale_pivots(first, make_coeffs(block_inverses[0], pivot_pattern[0], delays[0]))
    picked = jnp.take(first, PANEL + pivot_order[1], axis=0)
    second = jnp.take(widened[:, PANEL:], pivot_order[1], axis=1) - jnp.dot(scaled_one, picked.T, precision=lax.Precision.HIGHEST, preferred_element_type=jnp.float32)
    scaled_two = scale_pivots(second, make_coeffs(block_inverses[1], pivot_pattern[1], delays[1]))
    pivot_span = 2 * PANEL
    result = front_c - jnp.dot(scaled_one[pivot_span:], first[pivot_span:].T, precision=lax.Precision.HIGHEST, preferred_element_type=jnp.float32)
    result = result - jnp.dot(scaled_two[pivot_span:], second[pivot_span:].T, precision=lax.Precision.HIGHEST, preferred_element_type=jnp.float32)
    return result, second


def reference(old_tiles, remap, pivot_cols, pivot_order, pivot_pattern, block_inverses, delays):
    def advance(total, inputs):
        result, second = one_front(*inputs)
        return total + result, second

    total, seconds = lax.scan(advance, jnp.zeros((NC, NC), jnp.float32), (old_tiles, remap, pivot_cols, pivot_order, pivot_pattern, block_inverses, delays))
    return total.reshape(N_ROW, NC // N_ROW, NC), seconds
```

```python
import functools
import math

import jax
import jax.numpy as jnp
from jax import lax
from jax.experimental import pallas as pl
from jax.experimental.pallas import tpu as pltpu
from jax.sharding import PartitionSpec as P

CHUNKS = 4
BF = jnp.bfloat16
F32 = jnp.float32


def make_coeffs(inverses, pattern, delay, panel):
    half = panel // 2
    positions = jnp.arange(panel, dtype=jnp.int32)
    active = (positions < panel - delay).astype(F32)
    lo, hi = active[:half], active[half:]
    return jnp.stack(
        [inverses[0] * lo, inverses[1] * pattern.astype(F32) * lo * hi, inverses[2] * hi]
    )


def scaled(columns, coeffs):
    half = columns.shape[1] // 2
    left, right = columns[:, :half], columns[:, half:]
    one, off, two = coeffs[0:1], coeffs[1:2], coeffs[2:3]
    return jnp.concatenate([left * one + right * off, left * off + right * two], axis=1)


def split(value):
    high = lax.reduce_precision(value, 8, 7)
    return high.astype(BF), (value - high).astype(BF)


def ksplit(value):
    high = value.astype(BF)
    return high, (value - high.astype(F32)).astype(BF)


def nt(left, right):
    return lax.dot_general(left, right, (((1,), (1,)), ((), ())), preferred_element_type=F32)


def nn(left, right):
    return lax.dot_general(left, right, (((1,), (0,)), ((), ())), preferred_element_type=F32)


def route_kernel(source_ref, tile_ref, *out_refs):
    rows = out_refs[0].shape[1]
    for chunk, out_ref in enumerate(out_refs):
        out_ref[...] = tile_ref[:, chunk * rows : (chunk + 1) * rows, :]


def route_tiles(tiles, source, places):
    side = tiles.shape[1]
    rows = side // CHUNKS
    return pl.pallas_call(
        route_kernel,
        grid_spec=pltpu.PrefetchScalarGridSpec(
            num_scalar_prefetch=1,
            grid=(places,),
            in_specs=[pl.BlockSpec((1, side, side), lambda p, source: (source[p], 0, 0))],
            out_specs=[pl.BlockSpec((1, rows, side), lambda p, source: (p, 0, 0))] * CHUNKS,
        ),
        out_shape=[jax.ShapeDtypeStruct((places, rows, side), tiles.dtype)] * CHUNKS,
        compiler_params=pltpu.CompilerParams(vmem_limit_bytes=8 << 20),
        name="route",
    )(source, tiles)


def update_kernel(place_ref, order_ref, pivots_ref, coeffs_ref, cols_ref, rows_ref, out_ref, picked_ref, side_ref):
    panel = picked_ref.shape[0]

    def second_of(block):
        high, low = ksplit(scaled(block[:, :panel].astype(F32), coeffs_ref[0]))
        picked = picked_ref[...]
        return block[:, panel:].astype(F32) - (nt(high, picked) + nt(low, picked))

    @pl.when(pl.program_id(0) == 0)
    def _():
        spot = lax.broadcasted_iota(jnp.int32, (panel, panel), 1)
        choose = jnp.where(spot == order_ref[...], 1.0, 0.0).astype(BF)
        picked_ref[...] = nn(choose, pivots_ref[...]).astype(BF)
        step = min(256, cols_ref.shape[0])
        for at in range(0, cols_ref.shape[0], step):
            block = cols_ref[at : at + step, :]
            high, low = ksplit(scaled(block[:, :panel].astype(F32), coeffs_ref[0]))
            side_ref[at : at + step, 0:panel] = high
            side_ref[at : at + step, panel : 2 * panel] = low
            picked = picked_ref[...]
            second = block[:, panel:].astype(F32) - (nt(high, picked) + nt(low, picked))
            high, low = ksplit(scaled(second, coeffs_ref[1]))
            side_ref[at : at + step, 2 * panel : 3 * panel] = high
            side_ref[at : at + step, 3 * panel : 4 * panel] = low

    block = rows_ref[...]
    first = block[:, :panel]
    high, low = ksplit(second_of(block))
    total = nt(first, side_ref[:, 0:panel]) + nt(first, side_ref[:, panel : 2 * panel])
    total += nt(high, side_ref[:, 2 * panel : 3 * panel]) + nt(high, side_ref[:, 3 * panel : 4 * panel])
    total += nt(low, side_ref[:, 2 * panel : 3 * panel])
    out_ref[...] = total


def update(front, order, coeffs, row_index, col_index, row_span, col_span, panel):
    block = min(256, row_span)
    place = jnp.stack([(2 * panel + row_index * row_span) // block, (2 * panel + col_index * col_span) // col_span])
    width = 2 * panel
    return pl.pallas_call(
        update_kernel,
        grid_spec=pltpu.PrefetchScalarGridSpec(
            num_scalar_prefetch=1,
            grid=(row_span // block,),
            in_specs=[
                pl.BlockSpec((panel, 1), lambda i, place: (0, 0)),
                pl.BlockSpec((panel, panel), lambda i, place: (1, 0)),
                pl.BlockSpec(coeffs.shape, lambda i, place: (0, 0, 0)),
                pl.BlockSpec((col_span, width), lambda i, place: (place[1], 0)),
                pl.BlockSpec((block, width), lambda i, place: (place[0] + i, 0)),
            ],
            out_specs=pl.BlockSpec((block, col_span), lambda i, place: (i, 0)),
            scratch_shapes=[pltpu.VMEM((panel, panel), BF), pltpu.VMEM((col_span, 4 * panel), BF)],
        ),
        out_shape=jax.ShapeDtypeStruct((row_span, col_span), F32),
        compiler_params=pltpu.CompilerParams(vmem_limit_bytes=40 << 20),
        cost_estimate=pl.CostEstimate(
            flops=2 * row_span * col_span * 5 * panel, bytes_accessed=4 * row_span * col_span, transcendentals=0
        ),
        name="update",
    )(place, order[:, None], front, coeffs, front, front)


def collect_kernel(core_ref, starts_ref, listed_ref, tiles_ref, update_ref, away_ref, keep_ref):
    which, chip, pair = pl.program_id(0), pl.program_id(1), pl.program_id(2)
    pairs = pl.num_programs(2)
    core = core_ref[0]
    side = lax.select(which == 0, 1 - core, core)
    tile_row = (chip * 2 + side) * pairs + pair
    width = tiles_ref.shape[2]
    for column in range(update_ref.shape[3] // width):
        slot = tile_row * (update_ref.shape[3] // width) + column
        span = pl.ds(column * width, width)

        def add(k, total):
            return total + tiles_ref[listed_ref[k]].astype(F32)

        total = lax.fori_loop(starts_ref[slot], starts_ref[slot + 1], add, -update_ref[0, 0, :, span])

        @pl.when(which == 0)
        def _():
            away_ref[0, 0, :, span] = total

        @pl.when(which == 1)
        def _():
            keep_ref[0, 0, :, span] = total


def collect(core, starts, listed, tiles, update4, chunk, teams):
    tile_rows, _, rows, width = update4.shape
    chips, pairs = teams // 2, tile_rows // teams
    arrived = tiles.shape[0]

    def tile_row(which, chip, pair, core):
        side = lax.select(which == 0, 1 - core[0], core[0])
        return (chip * 2 + side) * pairs + pair

    def away(which, chip, pair, *_):
        return (lax.select(which == 0, chip, chips - 1), lax.select(which == 0, pair, pairs - 1), 0, 0)

    def keep(which, chip, pair, *_):
        return (lax.select(which == 0, 0, chip), lax.select(which == 0, 0, pair), 0, 0)

    shape = jax.ShapeDtypeStruct((chips, pairs, rows, width), F32)
    return pl.pallas_call(
        collect_kernel,
        grid_spec=pltpu.PrefetchScalarGridSpec(
            num_scalar_prefetch=3,
            grid=(2, chips, pairs),
            in_specs=[
                pl.BlockSpec((arrived, rows, tiles.shape[2]), lambda *_: (0, 0, 0)),
                pl.BlockSpec((1, 1, rows, width), lambda w, x, p, core, *_: (tile_row(w, x, p, core), chunk, 0, 0)),
            ],
            out_specs=[pl.BlockSpec((1, 1, rows, width), away), pl.BlockSpec((1, 1, rows, width), keep)],
        ),
        out_shape=[shape, shape],
        compiler_params=pltpu.CompilerParams(vmem_limit_bytes=12 << 20),
        name="collect",
    )(core, starts, listed, tiles, update4)


def covered(rows, panel, row_devices, col_devices):
    peers = row_devices * col_devices
    if row_devices != 2:
        return False
    contrib = rows * peers - 2 * panel
    row_span, col_span = contrib // row_devices, contrib // col_devices
    for r in range(row_devices):
        for c in range(col_devices):
            spans = [
                (panel, 2 * panel),
                (2 * panel + r * row_span, 2 * panel + (r + 1) * row_span),
                (2 * panel + c * col_span, 2 * panel + (c + 1) * col_span),
            ]
            needed = {s for low, high in spans for s in range(low // rows, (high - 1) // rows + 1)}
            line = {r * col_devices + k for k in range(col_devices)}
            crossed = [c - step if c >= step else c + step for step in range(col_devices)]
            line |= {(1 - r) * col_devices + k for k in crossed if k < col_devices}
            if not needed <= line:
                return False
    return True


def gather_front(own, row_index, col_index, row_devices, col_devices):
    rows, width = own.shape
    if not covered(rows, width // 2, row_devices, col_devices):
        return lax.all_gather(own, ("row", "col"), axis=0, tiled=True)
    spare = row_devices * col_devices
    front = jnp.zeros(((spare + 1) * rows, width), own.dtype)
    line = row_index * col_devices
    other = (1 - row_index) * col_devices
    swap = [(r, (r + 1) % row_devices) for r in range(row_devices)]

    def put(front, shard, index, valid):
        index = jnp.where(valid, index, spare)
        return lax.dynamic_update_slice(front, shard, (index * rows, 0))

    right = left = own
    crossing = own
    front = put(front, own, line + col_index, True)
    valid, crossed = True, col_index
    for step in range(1, col_devices + 1):
        if step < col_devices:
            ahead = [(i, i + 1) for i in range(step - 1, col_devices - 1)]
            right = lax.ppermute(right, "col", ahead)
            left = lax.ppermute(left, "col", [(col_devices - 1 - i, col_devices - 1 - j) for i, j in ahead])
        arrived = lax.ppermute(crossing, "row", swap)
        front = put(front, arrived, other + crossed, valid)
        if step < col_devices:
            behind = col_index >= step
            front = put(front, right, line + col_index - step, behind)
            front = put(front, left, line + col_index + step, col_index + step < col_devices)
            crossing = jnp.where(behind, right, left)
            crossed = jnp.where(behind, col_index - step, col_index + step)
            valid = crossed < col_devices
    return front


def local(old_tiles, remap, pivot_cols, pivot_order, pivot_pattern, block_inverses, delays):
    teams = lax.axis_size("team")
    row_devices = lax.axis_size("row")
    col_devices = lax.axis_size("col")
    peers = row_devices * col_devices
    row_index = lax.axis_index("row")
    col_index = lax.axis_index("col")
    core = lax.axis_index("team") % 2
    held = old_tiles.shape[1]
    side = old_tiles.shape[2]
    panel = pivot_order.shape[2]
    rows_here = pivot_cols.shape[1]
    contrib = rows_here * peers - 2 * panel
    tile_count = contrib // side
    row_span = contrib // row_devices
    col_span = contrib // col_devices
    per_row = row_span // side
    per_col = col_span // side
    slots_here = per_row * per_col

    orders = pivot_order[0]
    spot = jnp.arange(panel, dtype=jnp.int32)
    own_rows = pivot_cols[0]
    own = jnp.concatenate(
        [
            nn(own_rows[:, p * panel : (p + 1) * panel], (spot[:, None] == orders[p][None, :]).astype(BF)).astype(BF)
            for p in range(2)
        ],
        axis=1,
    )
    front = gather_front(own, row_index, col_index, row_devices, col_devices)

    targets = remap[0]
    tile_row = targets // tile_count
    tile_col = targets % tile_count
    owners = tile_row // per_row * col_devices + tile_col // per_col
    slots = tile_row % per_row * per_col + tile_col % per_col
    spread = min(peers, held // 2)
    capacity = (held + spread - 1) // spread
    indices = jnp.arange(held, dtype=jnp.int32)
    matched = (owners[:, None] == owners[None, :]) & (indices[None, :] < indices[:, None])
    ranks = jnp.sum(matched.astype(jnp.int32), axis=1)
    positions = owners * capacity + ranks
    places = peers * capacity
    routing = jnp.arange(places, dtype=jnp.int32)[:, None] == positions[None, :]
    source = jnp.sum(jnp.where(routing, indices[None, :], 0), axis=1)
    labels = jnp.sum(jnp.where(routing, slots[None, :] + 1, 0), axis=1) - 1
    send = functools.partial(
        lax.all_to_all, axis_name=("row", "col"), split_axis=0, concat_axis=0, tiled=True
    )
    outgoing = route_tiles(old_tiles[0], source, places)
    tags = send(labels)
    arrived = [send(part) for part in outgoing]
    keys = jnp.where(tags < 0, slots_here, tags)
    spots = jnp.arange(places, dtype=jnp.int32)
    before = (keys[None, :] < keys[:, None]) | ((keys[None, :] == keys[:, None]) & (spots[None, :] < spots[:, None]))
    order_of = jnp.sum(before.astype(jnp.int32), axis=1)
    listed = jnp.sum(jnp.where(spots[:, None] == order_of[None, :], spots[None, :], 0), axis=1)
    starts = jnp.sum((keys[None, :] < jnp.arange(slots_here + 1, dtype=jnp.int32)[:, None]).astype(jnp.int32), axis=1)

    coeffs = jnp.stack(
        [
            make_coeffs(block_inverses[0, p], pivot_pattern[0, p], delays[0, p], panel)
            for p in range(2)
        ]
    )
    change = update(front, orders[1], coeffs, row_index, col_index, row_span, col_span, panel)
    change = change.reshape(per_row, CHUNKS, side // CHUNKS, col_span)

    picked = nn(
        (spot[None, :] == orders[1][:, None]).astype(BF), lax.slice(front, (panel, 0), (2 * panel, panel))
    ).astype(BF)
    high, low = split(scaled(own[:, :panel].astype(F32), coeffs[0]))
    second = own[:, panel:].astype(F32) - (nt(high, picked) + nt(low, picked))

    chip = lax.axis_index("team") // 2
    cores = [(t, t // 2 * 2 + 1 - t % 2) for t in range(teams)]
    chips = [(t, (t + 2) % teams) for t in range(teams)]
    parts = []
    for chunk in range(CHUNKS):
        away, keep = collect(core[None], starts, listed, arrived[chunk], change, chunk, teams)
        both = keep + lax.ppermute(away, "team", cores)
        if teams == 4:
            far = lax.dynamic_index_in_dim(both, 1 - chip, 0, keepdims=False)
            near = lax.dynamic_index_in_dim(both, chip, 0, keepdims=False)
            parts.append(near + lax.ppermute(far, "team", chips))
        else:
            groups = [[t for t in range(teams) if t % 2 == c] for c in range(2)]
            parts.append(
                lax.psum_scatter(both, "team", scatter_dimension=0, axis_index_groups=groups, tiled=False)
            )
    parent = jnp.stack(parts, axis=1).reshape(row_span // teams, col_span)
    return (parent[None], second[None])


def solution(mesh):
    placed = (
        P("team", ("row", "col"), None, None),
        P("team", ("row", "col")),
        P("team", ("row", "col"), None),
        P("team", None, None),
        P("team", None, None),
        P("team", None, None, None),
        P("team", None),
    )
    return jax.shard_map(
        local,
        mesh=mesh,
        in_specs=placed,
        out_specs=(P("row", "team", "col"), P("team", ("row", "col"), None)),
        check_vma=False,
    )
```
